32 devices in a mesh: expert: 4 (over z), tensor: 8 (over y, x, core).
Axes of the slice: x: 2, y: 2, z: 4, core: 2. Of those that a mesh axis runs over, the one named last changes fastest.
Arguments:
- expert_inputs: bfloat16 [8, 64, 4096], P('expert'), may hold values from -6 to 6
- gates: float32 [8, 64], P('expert'), may hold values from 0.2 to 1
- chosen_tokens: int32 [8, 64], replicated, may hold values from 0 to 4095, as said below
- w_gate: bfloat16 [8, 4096, 1792], P('expert', None, 'tensor'), may hold values from -0.09375 to 0.09375
- w_up: bfloat16 [8, 4096, 1792], P('expert', None, 'tensor'), may hold values from -0.09375 to 0.09375
- w_down: bfloat16 [8, 1792, 4096], P('expert', 'tensor'), may hold values from -0.125 to 0.125
- residual: bfloat16 [4096, 4096], P(('expert', 'tensor')), may hold values from -6 to 6
- norm_gain: float32 [4096], replicated, may hold values from 0.5 to 1.5
- w_qkv: bfloat16 [4096, 12288], P(None, 'tensor'), may hold values from -0.09375 to 0.09375
Outputs:
- stream: bfloat16 [4096, 4096], P(('expert', 'tensor'))
- projected: bfloat16 [4096, 12288], P('expert', 'tensor')
The draws below stay inside these ranges and needn't reach their ends.
Inputs may be any that keep to these rules, and one draw needn't show every extreme that they name: `chosen_tokens`: each row holds 64 different token indices; at most 4 of a row lie in one block of 128 consecutive tokens, and in every draw some block holds 4 tokens of every row.
All inputs are finite; a program needn't handle non-finite values.
Results may differ from the reference program's by a relative error of at most 0.005.
Values may be sent and summed in bfloat16 or wider, within the bound.
A program may use at most 128 MiB of HBM per device.

```python
import jax
import jax.numpy as jnp
from jax import lax

D = 4096
FF = 1792
TOK_DEV = 128
MOST = 4
EXPERTS_LIVE = 8
CAP = 64
TOKENS = 4096


def draw_chosen_tokens(key, part):
    owner_total = TOKENS // TOK_DEV
    key_hot, key_forced, key_score, key_base = jax.random.split(jax.random.fold_in(key, 17), 4)
    popularity = jax.random.randint(key_hot, (owner_total,), 0, 4)
    mandatory_pick = jax.random.randint(key_forced, (), 0, owner_total)
    holder_numbers = jnp.arange(owner_total, dtype=jnp.int32)
    extra_score = popularity * 16384 + jnp.where(holder_numbers == mandatory_pick, 262144, 0)
    noise_term = jax.random.randint(key_score, (EXPERTS_LIVE, owner_total, MOST), 0, 65536)
    affinity_scores = noise_term + extra_score[None, :, None]
    ticket_ids = jnp.arange(owner_total * MOST, dtype=jnp.int32).reshape(1, owner_total, MOST)
    distinct = (affinity_scores * (owner_total * MOST) + ticket_ids).reshape(EXPERTS_LIVE, owner_total * MOST)
    picked_scores, picked = jax.lax.top_k(distinct, CAP)
    picked_owner = picked // MOST
    picked_rank = picked % MOST
    base_offset = jax.random.randint(key_base, (EXPERTS_LIVE, owner_total), 0, TOK_DEV)
    chosen_base = jnp.take_along_axis(base_offset, picked_owner, axis=1)
    offsets = (chosen_base + picked_rank) % TOK_DEV
    return (picked_owner * TOK_DEV + offsets).astype(jnp.int32)


def level_of(key, shape, shards, smallest, top_value):
    loudness, own = 1.0, jax.random.fold_in(key, 6)
    for axis_at, parts in shards:
        heights = jnp.exp(jax.random.uniform(jax.random.fold_in(own, axis_at), (parts,), jnp.float32, smallest / len(shards), top_value / len(shards)))
        loudness = loudness * jnp.repeat(heights, shape[axis_at] // parts).reshape([-1 if axis == axis_at else 1 for axis in range(len(shape))])
    return loudness


def normal_values(rng, extent, spread, most, cuts=(), held_as=jnp.bfloat16):
    entries = spread * jax.random.normal(rng, extent, jnp.float32)
    if cuts:
        entries = entries * level_of(rng, extent, cuts, -0.22, 0.18)
    return jnp.clip(entries, -most, most).astype(held_as)


def setup_inputs(seed: int = 0) -> dict:
    streams_of = jax.random.split(jax.random.key(seed), 10)
    expert_inputs = normal_values(streams_of[0], (EXPERTS_LIVE, CAP, D), 1.0, 6.0, ((0, 4),))
    gates = jnp.clip(0.2 + 0.8 * jax.random.uniform(streams_of[1], (EXPERTS_LIVE, CAP), jnp.float32) ** level_of(streams_of[1], (EXPERTS_LIVE, CAP), ((0, 4),), -0.2, 0.2), 0.2, 1.0)
    chosen_tokens = draw_chosen_tokens(jax.random.fold_in(streams_of[9], 71), 0)
    w_gate = normal_values(streams_of[3], (EXPERTS_LIVE, D, FF), D ** -0.5, 0.09375, ((0, 4), (2, 8)))
    w_up = normal_values(streams_of[4], (EXPERTS_LIVE, D, FF), D ** -0.5, 0.09375, ((0, 4), (2, 8)))
    w_down = normal_values(streams_of[5], (EXPERTS_LIVE, FF, D), FF ** -0.5, 0.125, ((0, 4), (1, 8)))
    residual = normal_values(streams_of[6], (TOKENS, D), 1.0, 6.0, ((0, 32),))
    norm_gain = jnp.clip(1.0 + 0.1 * jax.random.normal(streams_of[7], (D,), jnp.float32), 0.5, 1.5)
    w_qkv = normal_values(streams_of[8], (D, 3 * D), D ** -0.5, 0.09375, ((1, 8),))
    return {"expert_inputs": expert_inputs, "gates": gates, "chosen_tokens": chosen_tokens, "w_gate": w_gate, "w_up": w_up, "w_down": w_down, "residual": residual, "norm_gain": norm_gain, "w_qkv": w_qkv}


def expert_apply(operands):
    inputs_block, gate_block, gate_weight, up_weight, down_weight = operands
    gate_part = jnp.dot(inputs_block, gate_weight, preferred_element_type=jnp.float32)
    up_part = jnp.dot(inputs_block, up_weight, preferred_element_type=jnp.float32)
    hidden = (jax.nn.silu(gate_part) * up_part).astype(jnp.bfloat16)
    return jnp.dot(hidden, down_weight, preferred_element_type=jnp.float32) * gate_block[:, None]

def reference(expert_inputs, gates, chosen_tokens, w_gate, w_up, w_down, residual, norm_gain, w_qkv):
    expert_out = lax.map(expert_apply, (expert_inputs, gates, w_gate, w_up, w_down))
    scattered = jnp.zeros((TOKENS, D), jnp.float32).at[chosen_tokens.reshape(-1)].add(expert_out.reshape(-1, D))
    combined = residual.astype(jnp.float32) + scattered
    stream = combined.astype(jnp.bfloat16)
    scale_rows = lax.rsqrt(lax.optimization_barrier(jnp.mean(combined * combined, axis=-1, keepdims=True)) + 1e-06)
    normed = (combined * scale_rows * norm_gain[None, :]).astype(jnp.bfloat16)
    projected = jnp.dot(normed, w_qkv, preferred_element_type=jnp.float32).astype(jnp.bfloat16)
    return (stream, projected)
```

```python
import functools

import jax
import jax.numpy as jnp
from jax import lax
from jax.experimental import pallas as pl
from jax.experimental.pallas import tpu as pltpu
from jax.sharding import PartitionSpec as P

MOST = 4


def finish_kernel(
    row_steps,
    owner_ref,
    slots_ref,
    residual_ref,
    rows_ref,
    gain_ref,
    weight_ref,
    stream_ref,
    projected_ref,
    combined_ref,
    normed_ref,
):
    step = pl.program_id(0)
    tok_rows, feature_width = residual_ref.shape
    chunk = 512

    @pl.when(step < row_steps)
    def _():
        tokens = lax.broadcasted_iota(jnp.int32, (tok_rows, slots_ref.shape[1]), 0)
        placement = jnp.where(slots_ref[...] == tokens + step * tok_rows, 1.0, 0.0).astype(
            jnp.bfloat16
        )
        squares = jnp.zeros((tok_rows, 128), jnp.float32)
        for start in range(0, feature_width, chunk):
            cols = pl.ds(start, chunk)
            combined = residual_ref[:, cols].astype(jnp.float32) + jnp.dot(
                placement, rows_ref[:, cols], preferred_element_type=jnp.float32
            )
            combined_ref[:, cols] = combined
            for part in range(0, chunk, 128):
                piece = combined[:, part : part + 128]
                squares = squares + piece * piece
        mean = jnp.sum(squares, axis=1, keepdims=True) / feature_width
        scale = lax.rsqrt(mean + 1e-06)
        begin = pl.multiple_of(step * tok_rows, tok_rows)
        for start in range(0, feature_width, chunk):
            cols = pl.ds(start, chunk)
            normed_ref[pl.ds(begin, tok_rows), cols] = (
                combined_ref[:, cols] * scale * gain_ref[:, cols]
            ).astype(jnp.bfloat16)

        @pl.when(step == owner_ref[0])
        def _():
            stream_ref[...] = combined_ref[...].astype(jnp.bfloat16)

    @pl.when(step >= row_steps)
    def _():
        projected_ref[...] = jnp.dot(
            normed_ref[...], weight_ref[...], preferred_element_type=jnp.float32
        ).astype(jnp.bfloat16)


def finish(owner, slots, residual_all, rows, gain, w_qkv, tok_rows):
    total_rows, feature_width = residual_all.shape
    columns = w_qkv.shape[1]
    tile = 256
    row_steps = total_rows // tok_rows
    col_steps = columns // tile
    slot_total = rows.shape[0]
    return pl.pallas_call(
        functools.partial(finish_kernel, row_steps),
        grid=(row_steps + col_steps,),
        in_specs=[
            pl.BlockSpec(memory_space=pltpu.SMEM),
            pl.BlockSpec((1, slot_total), lambda i: (0, 0)),
            pl.BlockSpec((tok_rows, feature_width), lambda i: (jnp.minimum(i, row_steps - 1), 0)),
            pl.BlockSpec((slot_total, feature_width), lambda i: (0, 0)),
            pl.BlockSpec((1, feature_width), lambda i: (0, 0)),
            pl.BlockSpec((feature_width, tile), lambda i: (0, jnp.maximum(i - row_steps, 0))),
        ],
        out_specs=[
            pl.BlockSpec((tok_rows, feature_width), lambda i: (0, 0)),
            pl.BlockSpec((total_rows, tile), lambda i: (0, jnp.maximum(i - row_steps, 0))),
        ],
        out_shape=[
            jax.ShapeDtypeStruct((tok_rows, feature_width), jnp.bfloat16),
            jax.ShapeDtypeStruct((total_rows, columns), jnp.bfloat16),
        ],
        scratch_shapes=[
            pltpu.VMEM((tok_rows, feature_width), jnp.float32),
            pltpu.VMEM((total_rows, feature_width), jnp.bfloat16),
        ],
        compiler_params=pltpu.CompilerParams(
            vmem_limit_bytes=60 * 1024 * 1024, dimension_semantics=("arbitrary",)
        ),
        cost_estimate=pl.CostEstimate(
            flops=2 * total_rows * feature_width * (columns + slot_total),
            bytes_accessed=2 * (feature_width * columns + total_rows * columns),
            transcendentals=0,
        ),
    )(owner, slots, residual_all, rows, gain, w_qkv)


def per_device(
    expert_inputs, gates, chosen_tokens, w_gate, w_up, w_down, residual, norm_gain, w_qkv
):
    expert_count = lax.axis_size("expert")
    tensor_count = lax.axis_size("tensor")
    my_group = lax.axis_index("expert")
    local_experts, slot_count, feature_width = expert_inputs.shape
    tok_rows = residual.shape[0]
    group_rows = tok_rows * tensor_count
    keep = min(slot_count, MOST * tensor_count)

    residual_all = lax.all_gather(residual, "tensor", axis=0, tiled=True)

    dest = chosen_tokens // group_rows
    earlier = jnp.arange(slot_count)[None, :] < jnp.arange(slot_count)[:, None]
    rank = jnp.sum(
        ((dest[:, :, None] == dest[:, None, :]) & earlier[None]).astype(jnp.int32), axis=2
    )
    kept = jnp.arange(keep, dtype=jnp.int32)
    mine = jnp.where(dest == my_group, rank, -1)
    token_at = jnp.sum(
        jnp.where(
            mine[:, None, :] == kept[None, :, None],
            (chosen_tokens % group_rows)[:, None, :] + 1,
            0,
        ),
        axis=2,
    ).reshape(1, -1) - 1

    gate_part = jnp.einsum(
        "ecd,edf->ecf", expert_inputs, w_gate, preferred_element_type=jnp.float32
    )
    up_part = jnp.einsum("ecd,edf->ecf", expert_inputs, w_up, preferred_element_type=jnp.float32)
    hidden = (jax.nn.silu(gate_part) * up_part).astype(jnp.bfloat16)
    partial_value = (
        jnp.einsum("ecf,efd->ecd", hidden, w_down, preferred_element_type=jnp.float32)
        * gates[:, :, None]
    ).astype(jnp.bfloat16)
    row_total = local_experts * slot_count
    arrived = lax.all_to_all(
        partial_value.reshape(row_total, feature_width),
        "tensor",
        split_axis=1,
        concat_axis=0,
        tiled=True,
    ).reshape(tensor_count, local_experts, slot_count, -1)
    summed = jnp.sum(arrived.astype(jnp.float32), axis=0).astype(jnp.bfloat16)

    local_dest = lax.dynamic_slice_in_dim(dest, my_group * local_experts, local_experts, 0)
    local_rank = lax.dynamic_slice_in_dim(rank, my_group * local_experts, local_experts, 0)
    send_table = (
        (local_dest[None, :, None, :] == jnp.arange(expert_count)[:, None, None, None])
        & (local_rank[None, :, None, :] == kept[None, None, :, None])
    ).astype(jnp.bfloat16)
    outgoing = jnp.einsum("zlkj,ljf->zlkf", send_table, summed)
    incoming = lax.all_to_all(
        outgoing.reshape(expert_count, local_experts * keep, -1),
        "expert",
        split_axis=0,
        concat_axis=0,
        tiled=True,
    ).reshape(expert_count * local_experts * keep, -1)
    rows = lax.all_gather(incoming, "tensor", axis=1, tiled=True)

    return finish(
        lax.axis_index("tensor").reshape(1),
        token_at,
        residual_all,
        rows,
        norm_gain[None, :],
        w_qkv,
        tok_rows,
    )


def solution(mesh):
    return jax.shard_map(
        per_device,
        mesh=mesh,
        in_specs=(
            P("expert", None, None),
            P("expert", None),
            P(),
            P("expert", None, "tensor"),
            P("expert", None, "tensor"),
            P("expert", "tensor", None),
            P(("expert", "tensor"), None),
            P(),
            P(None, "tensor"),
        ),
        out_specs=(P(("expert", "tensor"), None), P("expert", "tensor")),
        check_vma=False,
    )
```

```python
import functools

import jax
import jax.numpy as jnp
from jax import lax
from jax.experimental import pallas as pl
from jax.experimental.pallas import tpu as pltpu
from jax.sharding import PartitionSpec as P

MOST = 4
MESH = pl.DeviceIdType.MESH


def finish_kernel(
    row_steps,
    order,
    owner_ref,
    slots_ref,
    residual_ref,
    rows_ref,
    gain_ref,
    weight_ref,
    stream_ref,
    projected_ref,
    combined_ref,
    normed_ref,
):
    step = pl.program_id(0)
    tok_rows, feature_width = residual_ref.shape
    chunk = rows_ref.shape[2]

    @pl.when(step < row_steps)
    def _():
        tokens = lax.broadcasted_iota(jnp.int32, (tok_rows, slots_ref.shape[1]), 0)
        placement = jnp.where(slots_ref[...] == tokens + step * tok_rows, 1.0, 0.0).astype(
            jnp.bfloat16
        )
        squares = jnp.zeros((tok_rows, 128), jnp.float32)
        for place, start in enumerate(range(0, feature_width, chunk)):
            cols = pl.ds(start, chunk)
            combined = residual_ref[:, cols].astype(jnp.float32) + jnp.dot(
                placement, rows_ref[order[place]], preferred_element_type=jnp.float32
            )
            combined_ref[:, cols] = combined
            for part in range(0, chunk, 128):
                piece = combined[:, part : part + 128]
                squares = squares + piece * piece
        mean = jnp.sum(squares, axis=1, keepdims=True) / feature_width
        scale = lax.rsqrt(mean + 1e-06)
        begin = pl.multiple_of(step * tok_rows, tok_rows)
        for start in range(0, feature_width, chunk):
            cols = pl.ds(start, chunk)
            normed_ref[pl.ds(begin, tok_rows), cols] = (
                combined_ref[:, cols] * scale * gain_ref[:, cols]
            ).astype(jnp.bfloat16)

        @pl.when(step == owner_ref[0])
        def _():
            stream_ref[...] = combined_ref[...].astype(jnp.bfloat16)

    @pl.when(step >= row_steps)
    def _():
        projected_ref[...] = jnp.dot(
            normed_ref[...], weight_ref[...], preferred_element_type=jnp.float32
        ).astype(jnp.bfloat16)


def finish(owner, slots, residual_all, rows, order, gain, w_qkv, tok_rows):
    total_rows, feature_width = residual_all.shape
    columns = w_qkv.shape[1]
    tile = 256
    row_steps = total_rows // tok_rows
    col_steps = columns // tile
    slot_total = rows.shape[1]
    return pl.pallas_call(
        functools.partial(finish_kernel, row_steps, order),
        grid=(row_steps + col_steps,),
        in_specs=[
            pl.BlockSpec(memory_space=pltpu.SMEM),
            pl.BlockSpec((1, slot_total), lambda i: (0, 0)),
            pl.BlockSpec((tok_rows, feature_width), lambda i: (jnp.minimum(i, row_steps - 1), 0)),
            pl.BlockSpec(rows.shape, lambda i: (0, 0, 0)),
            pl.BlockSpec((1, feature_width), lambda i: (0, 0)),
            pl.BlockSpec((feature_width, tile), lambda i: (0, jnp.maximum(i - row_steps, 0))),
        ],
        out_specs=[
            pl.BlockSpec((tok_rows, feature_width), lambda i: (0, 0)),
            pl.BlockSpec((total_rows, tile), lambda i: (0, jnp.maximum(i - row_steps, 0))),
        ],
        out_shape=[
            jax.ShapeDtypeStruct((tok_rows, feature_width), jnp.bfloat16),
            jax.ShapeDtypeStruct((total_rows, columns), jnp.bfloat16),
        ],
        scratch_shapes=[
            pltpu.VMEM((tok_rows, feature_width), jnp.float32),
            pltpu.VMEM((total_rows, feature_width), jnp.bfloat16),
        ],
        compiler_params=pltpu.CompilerParams(
            vmem_limit_bytes=60 * 1024 * 1024, dimension_semantics=("arbitrary",)
        ),
        cost_estimate=pl.CostEstimate(
            flops=2 * total_rows * feature_width * (columns + slot_total),
            bytes_accessed=2 * (feature_width * columns + total_rows * columns),
            transcendentals=0,
        ),
    )(owner, slots, residual_all, rows, gain, w_qkv)


def comm_kernel(
    groups,
    inputs_ref,
    gates_ref,
    table_ref,
    gate_hbm,
    up_hbm,
    down_hbm,
    residual_hbm,
    blocks_out,
    rows_out,
    gate_w,
    up_w,
    down_w,
    own,
    partial,
    half_in,
    chips_sum,
    chips_in,
    outgoing,
    slots_in,
    load_sem,
    first_send,
    first_recv,
    reduce_send,
    reduce_recv,
    group_send,
    group_recv,
    block_send,
    block_recv,
    row_send,
    row_recv,
    keep_sem,
):
    group = lax.axis_index("expert")
    me = lax.axis_index("tensor")
    core = me % 2
    partner = me + 1 - 2 * core
    along_x = me + 2 - 4 * ((me // 2) % 2)
    along_y = me + 4 - 8 * (me // 4)
    across = along_x + 4 - 8 * (me // 4)
    local_experts, slot_count, feature_width = inputs_ref.shape
    chips, row_total, width = chips_sum.shape

    def send(source, target, send_sem, recv_sem, device):
        copy = pltpu.make_async_remote_copy(
            src_ref=source,
            dst_ref=target,
            send_sem=send_sem,
            recv_sem=recv_sem,
            device_id=device,
            device_id_type=MESH,
        )
        copy.start()
        return copy

    loads = [pltpu.make_async_copy(residual_hbm, own, load_sem.at[0])]
    for index, (hbm, vmem) in enumerate(((gate_hbm, gate_w), (up_hbm, up_w), (down_hbm, down_w))):
        loads.append(pltpu.make_async_copy(hbm, vmem, load_sem.at[index + 1]))
    for copy in loads:
        copy.start()

    barrier = pltpu.get_barrier_semaphore()
    peers = [(group, device) for device in (partner, along_x, along_y, across)]
    peers += [((group + d) % groups, me) for d in range(1, groups)]
    for device in peers:
        pl.semaphore_signal(barrier, inc=1, device_id=device, device_id_type=MESH)
    pl.semaphore_wait(barrier, len(peers))

    def gather_parts(source, target, send_sem, recv_sem):
        half = source.shape[0] // 2
        parts = (pl.ds(0, half), pl.ds(half, half))

        def direct(which, device):
            role = 0 if device is along_x else 2
            return send(
                source.at[parts[which]],
                target.at[me, parts[which]],
                send_sem.at[role + which],
                recv_sem.at[role + which],
                (group, device),
            )

        def onward(which):
            origin, device = ((along_x, along_y), (along_y, along_x))[which]
            return send(
                target.at[origin, parts[which]],
                target.at[origin, parts[which]],
                send_sem.at[4 + which],
                recv_sem.at[4 + which],
                (group, device),
            )

        def to_partner(role, block):
            return send(
                block,
                target.at[(me, along_x, along_y, across)[role]],
                send_sem.at[6 + role],
                recv_sem.at[6 + role],
                (group, partner),
            )

        return direct, onward, to_partner

    block_direct, block_onward, block_partner = gather_parts(
        own, blocks_out, block_send, block_recv
    )
    row_direct, row_onward, row_partner = gather_parts(slots_in, rows_out, row_send, row_recv)

    loads[0].wait()
    block_x0 = block_direct(0, along_x)
    block_y1 = block_direct(1, along_y)
    block_own = block_partner(0, own)
    keep_block = pltpu.make_async_copy(own, blocks_out.at[me], keep_sem.at[0])
    keep_block.start()

    for copy in loads[1:]:
        copy.wait()
    contract = (((1,), (1,)), ((), ()))
    for expert in range(local_experts):
        gate_part = lax.dot_general(
            inputs_ref[expert], gate_w[expert], contract, preferred_element_type=jnp.float32
        )
        up_part = lax.dot_general(
            inputs_ref[expert], up_w[expert], contract, preferred_element_type=jnp.float32
        )
        hidden = (gate_part / (1.0 + jnp.exp(-gate_part)) * up_part).astype(jnp.bfloat16)
        lines = pl.ds(expert * slot_count, slot_count)
        for place in range(2 * chips):
            value = jnp.dot(
                hidden,
                down_w[expert, :, place * width : (place + 1) * width],
                preferred_element_type=jnp.float32,
            )
            partial[place, lines, :] = (value * gates_ref[expert]).astype(jnp.bfloat16)

    first = send(
        partial.at[pl.ds((1 - core) * chips, chips)],
        half_in,
        first_send,
        first_recv,
        (group, partner),
    )
    first.wait_recv()
    for chip in range(chips):
        chips_sum[chip] = (
            partial[core * chips + chip].astype(jnp.float32) + half_in[chip].astype(jnp.float32)
        ).astype(jnp.bfloat16)
    reduces = [
        send(
            chips_sum.at[device // 2],
            chips_in.at[index],
            reduce_send.at[index],
            reduce_recv.at[index],
            (group, device),
        )
        for index, device in enumerate((across, along_x, along_y))
    ]
    block_x1 = block_direct(1, along_x)
    block_y0 = block_direct(0, along_y)
    for copy in reduces:
        copy.wait_recv()
    total = chips_sum[me // 2].astype(jnp.float32)
    for index in range(3):
        total = total + chips_in[index].astype(jnp.float32)
    total = total.astype(jnp.bfloat16)
    for place in range(groups):
        outgoing[place] = jnp.dot(
            table_ref[place], total, preferred_element_type=jnp.float32
        ).astype(jnp.bfloat16)
    exchanges = [
        send(
            outgoing.at[(group + d) % groups],
            slots_in.at[group],
            group_send.at[d - 1],
            group_recv.at[d - 1],
            ((group + d) % groups, me),
        )
        for d in range(1, groups)
    ]
    slots_in[group] = outgoing[group]
    block_x0.wait_recv()
    block_o0 = block_onward(0)
    block_y1.wait_recv()
    block_o1 = block_onward(1)
    for copy in exchanges:
        copy.wait_recv()
    row_x0 = row_direct(0, along_x)
    row_y1 = row_direct(1, along_y)
    row_x1 = row_direct(1, along_x)
    row_y0 = row_direct(0, along_y)
    row_own = row_partner(0, slots_in)
    keep_rows = pltpu.make_async_copy(slots_in, rows_out.at[me], keep_sem.at[1])
    keep_rows.start()

    block_x1.wait_recv()
    block_px = block_partner(1, blocks_out.at[along_x])
    block_y0.wait_recv()
    block_py = block_partner(2, blocks_out.at[along_y])
    row_x0.wait_recv()
    row_o0 = row_onward(0)
    row_y1.wait_recv()
    row_o1 = row_onward(1)
    block_o0.wait_recv()
    block_o1.wait_recv()
    block_pd = block_partner(3, blocks_out.at[across])
    row_x1.wait_recv()
    row_px = row_partner(1, rows_out.at[along_x])
    row_y0.wait_recv()
    row_py = row_partner(2, rows_out.at[along_y])
    row_o0.wait_recv()
    row_o1.wait_recv()
    row_pd = row_partner(3, rows_out.at[across])

    keep_block.wait()
    keep_rows.wait()
    last = [block_own, block_px, block_py, block_pd, row_own, row_px, row_py, row_pd]
    for copy in last:
        copy.wait_recv()
    sent = last + reduces + exchanges + [first, block_x0, block_x1, block_y0, block_y1, block_o0]
    sent += [block_o1, row_x0, row_x1, row_y0, row_y1, row_o0, row_o1]
    for copy in sent:
        copy.wait_send()


def communicate(groups, members, table, inputs, gates, w_gate, w_up, w_down, residual):
    local_experts, slot_count, feature_width = inputs.shape
    tok_rows = residual.shape[0]
    row_total = local_experts * slot_count
    width = feature_width // members
    chips = members // 2
    keep = table.shape[1]
    bf16 = jnp.bfloat16
    anywhere = pl.BlockSpec(memory_space=pl.ANY)
    vmem = pl.BlockSpec(memory_space=pltpu.VMEM)
    dma = pltpu.SemaphoreType.DMA
    gate_t, up_t = jnp.swapaxes(w_gate, 1, 2), jnp.swapaxes(w_up, 1, 2)
    return pl.pallas_call(
        functools.partial(comm_kernel, groups),
        in_specs=[vmem, vmem, vmem, anywhere, anywhere, anywhere, anywhere],
        out_specs=[anywhere, anywhere],
        out_shape=[
            jax.ShapeDtypeStruct((members, tok_rows, feature_width), bf16),
            jax.ShapeDtypeStruct((members, groups, keep, width), bf16),
        ],
        scratch_shapes=[
            pltpu.VMEM(gate_t.shape, bf16),
            pltpu.VMEM(up_t.shape, bf16),
            pltpu.VMEM(w_down.shape, bf16),
            pltpu.VMEM((tok_rows, feature_width), bf16),
            pltpu.VMEM((members, row_total, width), bf16),
            pltpu.VMEM((chips, row_total, width), bf16),
            pltpu.VMEM((chips, row_total, width), bf16),
            pltpu.VMEM((chips - 1, row_total, width), bf16),
            pltpu.VMEM((groups, keep, width), bf16),
            pltpu.VMEM((groups, keep, width), bf16),
            dma((4,)),
            dma,
            dma,
            dma((3,)),
            dma((3,)),
            dma((groups - 1,)),
            dma((groups - 1,)),
            dma((10,)),
            dma((10,)),
            dma((10,)),
            dma((10,)),
            dma((2,)),
        ],
        compiler_params=pltpu.CompilerParams(
            collective_id=0, has_side_effects=True, vmem_limit_bytes=60 * 1024 * 1024
        ),
    )(inputs, gates[:, :, None], table, gate_t, up_t, w_down, residual)


def plain_rows(
    expert_inputs, gates, w_gate, w_up, w_down, send_table, expert_count, tensor_count
):
    local_experts, slot_count, feature_width = expert_inputs.shape
    gate_part = jnp.einsum(
        "ecd,edf->ecf", expert_inputs, w_gate, preferred_element_type=jnp.float32
    )
    up_part = jnp.einsum("ecd,edf->ecf", expert_inputs, w_up, preferred_element_type=jnp.float32)
    hidden = (jax.nn.silu(gate_part) * up_part).astype(jnp.bfloat16)
    partial_value = (
        jnp.einsum("ecf,efd->ecd", hidden, w_down, preferred_element_type=jnp.float32)
        * gates[:, :, None]
    ).astype(jnp.bfloat16)
    row_total = local_experts * slot_count
    arrived = lax.all_to_all(
        partial_value.reshape(row_total, feature_width),
        "tensor",
        split_axis=1,
        concat_axis=0,
        tiled=True,
    ).reshape(tensor_count, local_experts, slot_count, -1)
    summed = jnp.sum(arrived.astype(jnp.float32), axis=0).astype(jnp.bfloat16)

    outgoing = jnp.einsum("zlkmj,mjf->zlkf", send_table, summed)
    incoming = lax.all_to_all(
        outgoing.reshape(expert_count, -1, outgoing.shape[-1]),
        "expert",
        split_axis=0,
        concat_axis=0,
        tiled=True,
    )
    incoming = incoming.reshape(-1, outgoing.shape[-1])
    return lax.all_gather(incoming, "tensor", axis=0, tiled=False)


def per_device(
    expert_inputs, gates, chosen_tokens, w_gate, w_up, w_down, residual, norm_gain, w_qkv
):
    expert_count = lax.axis_size("expert")
    tensor_count = lax.axis_size("tensor")
    my_group = lax.axis_index("expert")
    local_experts, slot_count, feature_width = expert_inputs.shape
    tok_rows = residual.shape[0]
    group_rows = tok_rows * tensor_count
    keep = min(slot_count, MOST * tensor_count)

    dest = chosen_tokens // group_rows
    earlier = jnp.arange(slot_count)[None, :] < jnp.arange(slot_count)[:, None]
    rank = jnp.sum(
        ((dest[:, :, None] == dest[:, None, :]) & earlier[None]).astype(jnp.int32), axis=2
    )
    kept = jnp.arange(keep, dtype=jnp.int32)
    mine = jnp.where(dest == my_group, rank, -1)
    token_at = jnp.sum(
        jnp.where(
            mine[:, None, :] == kept[None, :, None],
            (chosen_tokens % group_rows)[:, None, :] + 1,
            0,
        ),
        axis=2,
    ).reshape(1, -1) - 1

    local_dest = lax.dynamic_slice_in_dim(dest, my_group * local_experts, local_experts, 0)
    local_rank = lax.dynamic_slice_in_dim(rank, my_group * local_experts, local_experts, 0)
    send_table = (
        (local_dest[None, :, None, :] == jnp.arange(expert_count)[:, None, None, None])
        & (local_rank[None, :, None, :] == kept[None, None, :, None])
    ).astype(jnp.bfloat16)
    same = jnp.eye(local_experts, dtype=jnp.bfloat16)
    send_table = send_table[:, :, :, None, :] * same[None, :, None, :, None]
    if tensor_count == 8:
        residual_all, rows = communicate(
            expert_count,
            tensor_count,
            send_table.reshape(expert_count, local_experts * keep, -1),
            expert_inputs,
            gates,
            w_gate,
            w_up,
            w_down,
            residual,
        )
        residual_all = residual_all.reshape(group_rows, feature_width)
        rows = rows.reshape(tensor_count, -1, feature_width // tensor_count)
        chips = tensor_count // 2
        order = tuple((c % chips) * 2 + c // chips for c in range(tensor_count))
    else:
        residual_all = lax.all_gather(residual, "tensor", axis=0, tiled=True)
        rows = plain_rows(
            expert_inputs, gates, w_gate, w_up, w_down, send_table, expert_count, tensor_count
        )
        order = tuple(range(tensor_count))

    return finish(
        lax.axis_index("tensor").reshape(1),
        token_at,
        residual_all,
        rows,
        order,
        norm_gain[None, :],
        w_qkv,
        tok_rows,
    )


def solution(mesh):
    return jax.shard_map(
        per_device,
        mesh=mesh,
        in_specs=(
            P("expert", None, None),
            P("expert", None),
            P(),
            P("expert", None, "tensor"),
            P("expert", None, "tensor"),
            P("expert", "tensor", None),
            P(("expert", "tensor"), None),
            P(),
            P(None, "tensor"),
        ),
        out_specs=(P(("expert", "tensor"), None), P("expert", "tensor")),
        check_vma=False,
    )
```

```python
import functools

import jax
import jax.numpy as jnp
from jax import lax
from jax.experimental import pallas as pl
from jax.experimental.pallas import tpu as pltpu
from jax.sharding import PartitionSpec as P

MOST = 4
MESH = pl.DeviceIdType.MESH


def finish_kernel(
    row_steps,
    order,
    owner_ref,
    slots_ref,
    residual_ref,
    rows_ref,
    gain_ref,
    weight_ref,
    stream_ref,
    projected_ref,
    combined_ref,
    normed_ref,
):
    step = pl.program_id(0)
    tok_rows, feature_width = residual_ref.shape
    chunk = rows_ref.shape[2]

    @pl.when(step < row_steps)
    def _():
        tokens = lax.broadcasted_iota(jnp.int32, (tok_rows, slots_ref.shape[1]), 0)
        placement = jnp.where(slots_ref[...] == tokens + step * tok_rows, 1.0, 0.0).astype(
            jnp.bfloat16
        )
        squares = jnp.zeros((tok_rows, 128), jnp.float32)
        for place, start in enumerate(range(0, feature_width, chunk)):
            cols = pl.ds(start, chunk)
            combined = residual_ref[:, cols].astype(jnp.float32) + jnp.dot(
                placement, rows_ref[order[place]], preferred_element_type=jnp.float32
            )
            combined_ref[:, cols] = combined
            for part in range(0, chunk, 128):
                piece = combined[:, part : part + 128]
                squares = squares + piece * piece
        mean = jnp.sum(squares, axis=1, keepdims=True) / feature_width
        scale = lax.rsqrt(mean + 1e-06)
        begin = pl.multiple_of(step * tok_rows, tok_rows)
        for start in range(0, feature_width, chunk):
            cols = pl.ds(start, chunk)
            normed_ref[pl.ds(begin, tok_rows), cols] = (
                combined_ref[:, cols] * scale * gain_ref[:, cols]
            ).astype(jnp.bfloat16)

        @pl.when(step == owner_ref[0])
        def _():
            stream_ref[...] = combined_ref[...].astype(jnp.bfloat16)

    @pl.when(step >= row_steps)
    def _():
        projected_ref[...] = jnp.dot(
            normed_ref[...], weight_ref[...], preferred_element_type=jnp.float32
        ).astype(jnp.bfloat16)


def finish(owner, slots, residual_all, rows, order, gain, w_qkv, tok_rows):
    total_rows, feature_width = residual_all.shape
    columns = w_qkv.shape[1]
    tile = 256
    row_steps = total_rows // tok_rows
    col_steps = columns // tile
    slot_total = rows.shape[1]
    return pl.pallas_call(
        functools.partial(finish_kernel, row_steps, order),
        grid=(row_steps + col_steps,),
        in_specs=[
            pl.BlockSpec(memory_space=pltpu.SMEM),
            pl.BlockSpec((1, slot_total), lambda i: (0, 0)),
            pl.BlockSpec((tok_rows, feature_width), lambda i: (jnp.minimum(i, row_steps - 1), 0)),
            pl.BlockSpec(rows.shape, lambda i: (0, 0, 0)),
            pl.BlockSpec((1, feature_width), lambda i: (0, 0)),
            pl.BlockSpec((feature_width, tile), lambda i: (0, jnp.maximum(i - row_steps, 0))),
        ],
        out_specs=[
            pl.BlockSpec((tok_rows, feature_width), lambda i: (0, 0)),
            pl.BlockSpec((total_rows, tile), lambda i: (0, jnp.maximum(i - row_steps, 0))),
        ],
        out_shape=[
            jax.ShapeDtypeStruct((tok_rows, feature_width), jnp.bfloat16),
            jax.ShapeDtypeStruct((total_rows, columns), jnp.bfloat16),
        ],
        scratch_shapes=[
            pltpu.VMEM((tok_rows, feature_width), jnp.float32),
            pltpu.VMEM((total_rows, feature_width), jnp.bfloat16),
        ],
        compiler_params=pltpu.CompilerParams(
            vmem_limit_bytes=60 * 1024 * 1024, dimension_semantics=("arbitrary",)
        ),
        cost_estimate=pl.CostEstimate(
            flops=2 * total_rows * feature_width * (columns + slot_total),
            bytes_accessed=2 * (feature_width * columns + total_rows * columns),
            transcendentals=0,
        ),
    )(owner, slots, residual_all, rows, gain, w_qkv)


def comm_kernel(
    groups,
    inputs_ref,
    gates_ref,
    table_ref,
    gate_hbm,
    up_hbm,
    down_hbm,
    residual_hbm,
    slots_ref,
    gain_ref,
    weight_hbm,
    stream_ref,
    projected_hbm,
    gate_w,
    up_w,
    down_w,
    weight,
    blocks,
    rows,
    combined_ref,
    normed_ref,
    staged,
    partial,
    half_in,
    chips_sum,
    chips_in,
    outgoing,
    load_sem,
    first_send,
    first_recv,
    reduce_send,
    reduce_recv,
    group_send,
    group_recv,
    block_send,
    block_recv,
    row_send,
    row_recv,
    store_sem,
):
    group = lax.axis_index("expert")
    me = lax.axis_index("tensor")
    core = me % 2
    partner = me + 1 - 2 * core
    along_x = me + 2 - 4 * ((me // 2) % 2)
    along_y = me + 4 - 8 * (me // 4)
    across = along_x + 4 - 8 * (me // 4)
    local_experts, slot_count, feature_width = inputs_ref.shape
    chips, row_total, width = chips_sum.shape

    def send(source, target, send_sem, recv_sem, device):
        copy = pltpu.make_async_remote_copy(
            src_ref=source,
            dst_ref=target,
            send_sem=send_sem,
            recv_sem=recv_sem,
            device_id=device,
            device_id_type=MESH,
        )
        copy.start()
        return copy

    tok_rows = residual_hbm.shape[0]
    loads = [pltpu.make_async_copy(residual_hbm, blocks.at[me], load_sem.at[0])]
    for index, (hbm, vmem) in enumerate(((gate_hbm, gate_w), (up_hbm, up_w), (down_hbm, down_w))):
        loads.append(pltpu.make_async_copy(hbm, vmem, load_sem.at[index + 1]))
    for copy in loads:
        copy.start()
    load_weight = pltpu.make_async_copy(weight_hbm, weight, load_sem.at[4])
    load_weight.start()

    barrier = pltpu.get_barrier_semaphore()
    peers = [(group, device) for device in (partner, along_x, along_y, across)]
    peers += [((group + d) % groups, me) for d in range(1, groups)]
    for device in peers:
        pl.semaphore_signal(barrier, inc=1, device_id=device, device_id_type=MESH)
    pl.semaphore_wait(barrier, len(peers))

    half, quarter, groups_half = tok_rows // 2, tok_rows // 4, groups // 2
    corner = (me, along_x, along_y, across)

    def block_send_to(index, origin, start, size, device):
        part = blocks.at[origin, pl.ds(start, size)]
        return send(part, part, block_send.at[index], block_recv.at[index], (group, device))

    def row_send_to(index, origin, start, size, device):
        part = rows.at[origin, pl.ds(start, size)]
        return send(part, part, row_send.at[index], row_recv.at[index], (group, device))

    def block_partner(role):
        return block_send_to(8 + role, corner[role], 0, tok_rows, partner)

    def row_partner(role):
        return row_send_to(6 + role, corner[role], 0, groups, partner)

    loads[0].wait()
    block_x0 = block_send_to(0, me, 0, half, along_x)
    block_y0 = block_send_to(1, me, half, half, along_y)
    block_own = block_partner(0)

    for copy in loads[1:]:
        copy.wait()
    contract = (((1,), (1,)), ((), ()))
    for expert in range(local_experts):
        gate_part = lax.dot_general(
            inputs_ref[expert], gate_w[expert], contract, preferred_element_type=jnp.float32
        )
        up_part = lax.dot_general(
            inputs_ref[expert], up_w[expert], contract, preferred_element_type=jnp.float32
        )
        hidden = (gate_part / (1.0 + jnp.exp(-gate_part)) * up_part).astype(jnp.bfloat16)
        lines = pl.ds(expert * slot_count, slot_count)
        for place in range(2 * chips):
            value = jnp.dot(
                hidden,
                down_w[expert, :, place * width : (place + 1) * width],
                preferred_element_type=jnp.float32,
            )
            partial[place, lines, :] = (value * gates_ref[expert]).astype(jnp.bfloat16)

    first = send(
        partial.at[pl.ds((1 - core) * chips, chips)],
        half_in,
        first_send,
        first_recv,
        (group, partner),
    )
    first.wait_recv()
    for chip in range(chips):
        chips_sum[chip] = (
            partial[core * chips + chip].astype(jnp.float32) + half_in[chip].astype(jnp.float32)
        ).astype(jnp.bfloat16)
    reduces = [
        send(
            chips_sum.at[device // 2],
            chips_in.at[index],
            reduce_send.at[index],
            reduce_recv.at[index],
            (group, device),
        )
        for index, device in enumerate((across, along_x, along_y))
    ]
    block_x1 = block_send_to(2, me, half, quarter, along_x)
    block_y1 = block_send_to(3, me, 0, quarter, along_y)
    for copy in reduces:
        copy.wait_recv()
    total = chips_sum[me // 2].astype(jnp.float32)
    for index in range(3):
        total = total + chips_in[index].astype(jnp.float32)
    total = total.astype(jnp.bfloat16)
    for place in range(groups):
        outgoing[place] = jnp.dot(
            table_ref[place], total, preferred_element_type=jnp.float32
        ).astype(jnp.bfloat16)
    exchanges = [
        send(
            outgoing.at[(group + d) % groups],
            rows.at[me, group],
            group_send.at[d - 1],
            group_recv.at[d - 1],
            ((group + d) % groups, me),
        )
        for d in range(1, groups)
    ]
    rows[me, group] = outgoing[group]
    for copy in exchanges:
        copy.wait_recv()
    rest = groups - groups_half
    row_x0 = row_send_to(0, me, 0, groups_half, along_x)
    row_y0 = row_send_to(1, me, groups_half, rest, along_y)
    row_x1 = row_send_to(2, me, groups_half, rest, along_x)
    row_y1 = row_send_to(3, me, 0, groups_half, along_y)
    row_own = row_partner(0)
    row_x0.wait_recv()
    row_ox = row_send_to(4, along_x, 0, groups_half, along_y)
    row_y0.wait_recv()
    row_oy = row_send_to(5, along_y, groups_half, rest, along_x)
    block_x2 = block_send_to(4, me, half + quarter, quarter, along_x)
    block_y2 = block_send_to(5, me, quarter, quarter, along_y)
    block_x0.wait_recv()
    block_ox = block_send_to(6, along_x, 0, half, along_y)
    block_y0.wait_recv()
    block_oy = block_send_to(7, along_y, half, half, along_x)
    row_x1.wait_recv()
    row_px = row_partner(1)
    row_y1.wait_recv()
    row_py = row_partner(2)
    row_ox.wait_recv()
    row_oy.wait_recv()
    row_pd = row_partner(3)
    block_own.wait_recv()
    for copy in (row_own, row_px, row_py, row_pd):
        copy.wait_recv()
    load_weight.wait()

    pair = 2 * tok_rows
    slot_total = slots_ref.shape[1]
    tile = 256
    col_tiles = weight.shape[1] // tile
    stores = []

    def finish_pair(step, chip):
        def place(index, squares):
            cols = pl.ds(pl.multiple_of(index * width, width), width)
            tokens = lax.broadcasted_iota(jnp.int32, (pair, slot_total), 0) + chip * pair
            placement = jnp.where(slots_ref[...] == tokens, 1.0, 0.0).astype(jnp.bfloat16)
            source = (index % chips) * 2 + index // chips
            values = rows[source].reshape(slot_total, width)
            block = blocks[pl.ds(2 * chip, 2), :, cols].reshape(pair, width)
            combined = block.astype(jnp.float32) + jnp.dot(
                placement, values, preferred_element_type=jnp.float32
            )
            combined_ref[:, cols] = combined
            for part in range(0, width, 128):
                piece = combined[:, part : part + 128]
                squares = squares + piece * piece
            return squares

        squares = lax.fori_loop(0, 2 * chips, place, jnp.zeros((pair, 128), jnp.float32))
        scale = lax.rsqrt(jnp.sum(squares, axis=1, keepdims=True) / feature_width + 1e-06)

        def norm(index, carry):
            cols = pl.ds(pl.multiple_of(index * width, width), width)
            normed_ref[:, cols] = (combined_ref[:, cols] * scale * gain_ref[:, cols]).astype(
                jnp.bfloat16
            )
            return carry

        lax.fori_loop(0, 2 * chips, norm, 0)
        if step == 0:
            begin = pl.multiple_of(core * tok_rows, tok_rows)
            stream_ref[...] = combined_ref[pl.ds(begin, tok_rows), :].astype(jnp.bfloat16)

        def project(index, carry):
            cols = pl.ds(pl.multiple_of(index * tile, tile), tile)
            staged[step, :, cols] = jnp.dot(
                normed_ref[...], weight[:, cols], preferred_element_type=jnp.float32
            ).astype(jnp.bfloat16)
            return carry

        lax.fori_loop(0, col_tiles, project, 0)
        begin = pl.multiple_of(chip * pair, pair)
        store = pltpu.make_async_copy(
            staged.at[step], projected_hbm.at[pl.ds(begin, pair)], store_sem.at[step]
        )
        store.start()
        stores.append(store)

    finish_pair(0, me // 2)
    block_x1.wait_recv()
    block_x2.wait_recv()
    block_px = block_partner(1)
    block_y1.wait_recv()
    block_y2.wait_recv()
    block_py = block_partner(2)
    block_px.wait_recv()
    finish_pair(1, along_x // 2)
    block_ox.wait_recv()
    block_oy.wait_recv()
    block_pd = block_partner(3)
    block_py.wait_recv()
    finish_pair(2, along_y // 2)
    block_pd.wait_recv()
    finish_pair(3, across // 2)

    sent = [block_own, block_px, block_py, block_pd, row_own, row_px, row_py, row_pd]
    sent += reduces + exchanges + [first, block_x0, block_x1, block_x2]
    sent += [block_y0, block_y1, block_y2, block_ox, block_oy]
    sent += [row_x0, row_x1, row_y0, row_y1, row_ox, row_oy]
    for copy in sent:
        copy.wait_send()
    for store in stores:
        store.wait()


def communicate(
    groups, members, table, inputs, gates, w_gate, w_up, w_down, residual, slots, gain, w_qkv
):
    local_experts, slot_count, feature_width = inputs.shape
    tok_rows = residual.shape[0]
    row_total = local_experts * slot_count
    width = feature_width // members
    chips = members // 2
    keep = table.shape[1]
    bf16 = jnp.bfloat16
    anywhere = pl.BlockSpec(memory_space=pl.ANY)
    vmem = pl.BlockSpec(memory_space=pltpu.VMEM)
    dma = pltpu.SemaphoreType.DMA
    gate_t, up_t = jnp.swapaxes(w_gate, 1, 2), jnp.swapaxes(w_up, 1, 2)
    return pl.pallas_call(
        functools.partial(comm_kernel, groups),
        in_specs=[vmem] * 3 + [anywhere] * 4 + [vmem, vmem, anywhere],
        out_specs=[vmem, anywhere],
        out_shape=[
            jax.ShapeDtypeStruct((tok_rows, feature_width), bf16),
            jax.ShapeDtypeStruct((members * tok_rows, w_qkv.shape[1]), bf16),
        ],
        scratch_shapes=[
            pltpu.VMEM(gate_t.shape, bf16),
            pltpu.VMEM(up_t.shape, bf16),
            pltpu.VMEM(w_down.shape, bf16),
            pltpu.VMEM(w_qkv.shape, bf16),
            pltpu.VMEM((members, tok_rows, feature_width), bf16),
            pltpu.VMEM((members, groups, keep, width), bf16),
            pltpu.VMEM((2 * tok_rows, feature_width), jnp.float32),
            pltpu.VMEM((2 * tok_rows, feature_width), bf16),
            pltpu.VMEM((chips, 2 * tok_rows, w_qkv.shape[1]), bf16),
            pltpu.VMEM((members, row_total, width), bf16),
            pltpu.VMEM((chips, row_total, width), bf16),
            pltpu.VMEM((chips, row_total, width), bf16),
            pltpu.VMEM((chips - 1, row_total, width), bf16),
            pltpu.VMEM((groups, keep, width), bf16),
            dma((5,)),
            dma,
            dma,
            dma((3,)),
            dma((3,)),
            dma((groups - 1,)),
            dma((groups - 1,)),
            dma((12,)),
            dma((12,)),
            dma((10,)),
            dma((10,)),
            dma((chips,)),
        ],
        compiler_params=pltpu.CompilerParams(
            collective_id=0, has_side_effects=True, vmem_limit_bytes=60 * 1024 * 1024
        ),
    )(inputs, gates[:, :, None], table, gate_t, up_t, w_down, residual, slots, gain, w_qkv)


def plain_rows(
    expert_inputs, gates, w_gate, w_up, w_down, send_table, expert_count, tensor_count
):
    local_experts, slot_count, feature_width = expert_inputs.shape
    gate_part = jnp.einsum(
        "ecd,edf->ecf", expert_inputs, w_gate, preferred_element_type=jnp.float32
    )
    up_part = jnp.einsum("ecd,edf->ecf", expert_inputs, w_up, preferred_element_type=jnp.float32)
    hidden = (jax.nn.silu(gate_part) * up_part).astype(jnp.bfloat16)
    partial_value = (
        jnp.einsum("ecf,efd->ecd", hidden, w_down, preferred_element_type=jnp.float32)
        * gates[:, :, None]
    ).astype(jnp.bfloat16)
    row_total = local_experts * slot_count
    arrived = lax.all_to_all(
        partial_value.reshape(row_total, feature_width),
        "tensor",
        split_axis=1,
        concat_axis=0,
        tiled=True,
    ).reshape(tensor_count, local_experts, slot_count, -1)
    summed = jnp.sum(arrived.astype(jnp.float32), axis=0).astype(jnp.bfloat16)

    outgoing = jnp.einsum("zlkmj,mjf->zlkf", send_table, summed)
    incoming = lax.all_to_all(
        outgoing.reshape(expert_count, -1, outgoing.shape[-1]),
        "expert",
        split_axis=0,
        concat_axis=0,
        tiled=True,
    )
    incoming = incoming.reshape(-1, outgoing.shape[-1])
    return lax.all_gather(incoming, "tensor", axis=0, tiled=False)


def per_device(
    expert_inputs, gates, chosen_tokens, w_gate, w_up, w_down, residual, norm_gain, w_qkv
):
    expert_count = lax.axis_size("expert")
    tensor_count = lax.axis_size("tensor")
    my_group = lax.axis_index("expert")
    local_experts, slot_count, feature_width = expert_inputs.shape
    tok_rows = residual.shape[0]
    group_rows = tok_rows * tensor_count
    keep = min(slot_count, MOST * tensor_count)

    dest = chosen_tokens // group_rows
    earlier = jnp.arange(slot_count)[None, :] < jnp.arange(slot_count)[:, None]
    rank = jnp.sum(
        ((dest[:, :, None] == dest[:, None, :]) & earlier[None]).astype(jnp.int32), axis=2
    )
    kept = jnp.arange(keep, dtype=jnp.int32)
    mine = jnp.where(dest == my_group, rank, -1)
    token_at = jnp.sum(
        jnp.where(
            mine[:, None, :] == kept[None, :, None],
            (chosen_tokens % group_rows)[:, None, :] + 1,
            0,
        ),
        axis=2,
    ).reshape(1, -1) - 1

    local_dest = lax.dynamic_slice_in_dim(dest, my_group * local_experts, local_experts, 0)
    local_rank = lax.dynamic_slice_in_dim(rank, my_group * local_experts, local_experts, 0)
    send_table = (
        (local_dest[None, :, None, :] == jnp.arange(expert_count)[:, None, None, None])
        & (local_rank[None, :, None, :] == kept[None, None, :, None])
    ).astype(jnp.bfloat16)
    same = jnp.eye(local_experts, dtype=jnp.bfloat16)
    send_table = send_table[:, :, :, None, :] * same[None, :, None, :, None]
    if tensor_count == 8:
        return communicate(
            expert_count,
            tensor_count,
            send_table.reshape(expert_count, local_experts * keep, -1),
            expert_inputs,
            gates,
            w_gate,
            w_up,
            w_down,
            residual,
            token_at,
            norm_gain[None, :],
            w_qkv,
        )
    residual_all = lax.all_gather(residual, "tensor", axis=0, tiled=True)
    rows = plain_rows(
        expert_inputs, gates, w_gate, w_up, w_down, send_table, expert_count, tensor_count
    )
    order = tuple(range(tensor_count))
    return finish(
        lax.axis_index("tensor").reshape(1),
        token_at,
        residual_all,
        rows,
        order,
        norm_gain[None, :],
        w_qkv,
        tok_rows,
    )


def solution(mesh):
    return jax.shard_map(
        per_device,
        mesh=mesh,
        in_specs=(
            P("expert", None, None),
            P("expert", None),
            P(),
            P("expert", None, "tensor"),
            P("expert", None, "tensor"),
            P("expert", "tensor", None),
            P(("expert", "tensor"), None),
            P(),
            P(None, "tensor"),
        ),
        out_specs=(P(("expert", "tensor"), None), P("expert", "tensor")),
        check_vma=False,
    )
```

```python
import functools

import jax
import jax.numpy as jnp
from jax import lax
from jax.experimental import pallas as pl
from jax.experimental.pallas import tpu as pltpu
from jax.sharding import PartitionSpec as P

MOST = 4
MESH = pl.DeviceIdType.MESH


def finish_kernel(
    row_steps,
    order,
    owner_ref,
    slots_ref,
    residual_ref,
    rows_ref,
    gain_ref,
    weight_ref,
    stream_ref,
    projected_ref,
    combined_ref,
    normed_ref,
):
    step = pl.program_id(0)
    tok_rows, feature_width = residual_ref.shape
    chunk = rows_ref.shape[2]

    @pl.when(step < row_steps)
    def _():
        tokens = lax.broadcasted_iota(jnp.int32, (tok_rows, slots_ref.shape[1]), 0)
        placement = jnp.where(slots_ref[...] == tokens + step * tok_rows, 1.0, 0.0).astype(
            jnp.bfloat16
        )
        squares = jnp.zeros((tok_rows, 128), jnp.float32)
        for place, start in enumerate(range(0, feature_width, chunk)):
            cols = pl.ds(start, chunk)
            combined = residual_ref[:, cols].astype(jnp.float32) + jnp.dot(
                placement, rows_ref[order[place]], preferred_element_type=jnp.float32
            )
            combined_ref[:, cols] = combined
            for part in range(0, chunk, 128):
                piece = combined[:, part : part + 128]
                squares = squares + piece * piece
        mean = jnp.sum(squares, axis=1, keepdims=True) / feature_width
        scale = lax.rsqrt(mean + 1e-06)
        begin = pl.multiple_of(step * tok_rows, tok_rows)
        for start in range(0, feature_width, chunk):
            cols = pl.ds(start, chunk)
            normed_ref[pl.ds(begin, tok_rows), cols] = (
                combined_ref[:, cols] * scale * gain_ref[:, cols]
            ).astype(jnp.bfloat16)

        @pl.when(step == owner_ref[0])
        def _():
            stream_ref[...] = combined_ref[...].astype(jnp.bfloat16)

    @pl.when(step >= row_steps)
    def _():
        projected_ref[...] = jnp.dot(
            normed_ref[...], weight_ref[...], preferred_element_type=jnp.float32
        ).astype(jnp.bfloat16)


def finish(owner, slots, residual_all, rows, order, gain, w_qkv, tok_rows):
    total_rows, feature_width = residual_all.shape
    columns = w_qkv.shape[1]
    tile = 256
    row_steps = total_rows // tok_rows
    col_steps = columns // tile
    slot_total = rows.shape[1]
    return pl.pallas_call(
        functools.partial(finish_kernel, row_steps, order),
        grid=(row_steps + col_steps,),
        in_specs=[
            pl.BlockSpec(memory_space=pltpu.SMEM),
            pl.BlockSpec((1, slot_total), lambda i: (0, 0)),
            pl.BlockSpec((tok_rows, feature_width), lambda i: (jnp.minimum(i, row_steps - 1), 0)),
            pl.BlockSpec(rows.shape, lambda i: (0, 0, 0)),
            pl.BlockSpec((1, feature_width), lambda i: (0, 0)),
            pl.BlockSpec((feature_width, tile), lambda i: (0, jnp.maximum(i - row_steps, 0))),
        ],
        out_specs=[
            pl.BlockSpec((tok_rows, feature_width), lambda i: (0, 0)),
            pl.BlockSpec((total_rows, tile), lambda i: (0, jnp.maximum(i - row_steps, 0))),
        ],
        out_shape=[
            jax.ShapeDtypeStruct((tok_rows, feature_width), jnp.bfloat16),
            jax.ShapeDtypeStruct((total_rows, columns), jnp.bfloat16),
        ],
        scratch_shapes=[
            pltpu.VMEM((tok_rows, feature_width), jnp.float32),
            pltpu.VMEM((total_rows, feature_width), jnp.bfloat16),
        ],
        compiler_params=pltpu.CompilerParams(
            vmem_limit_bytes=60 * 1024 * 1024, dimension_semantics=("arbitrary",)
        ),
        cost_estimate=pl.CostEstimate(
            flops=2 * total_rows * feature_width * (columns + slot_total),
            bytes_accessed=2 * (feature_width * columns + total_rows * columns),
            transcendentals=0,
        ),
    )(owner, slots, residual_all, rows, gain, w_qkv)


def comm_kernel(
    groups,
    inputs_ref,
    gates_ref,
    table_ref,
    gate_hbm,
    up_hbm,
    down_hbm,
    residual_hbm,
    slots_ref,
    gain_ref,
    weight_hbm,
    stream_ref,
    projected_hbm,
    gate_w,
    up_w,
    down_w,
    weight,
    blocks,
    rows,
    combined_ref,
    normed_ref,
    staged,
    partial,
    half_in,
    chips_sum,
    chips_in,
    outgoing,
    load_sem,
    first_send,
    first_recv,
    reduce_send,
    reduce_recv,
    group_send,
    group_recv,
    block_send,
    block_recv,
    row_send,
    row_recv,
    store_sem,
):
    group = lax.axis_index("expert")
    me = lax.axis_index("tensor")
    core = me % 2
    partner = me + 1 - 2 * core
    along_x = me + 2 - 4 * ((me // 2) % 2)
    along_y = me + 4 - 8 * (me // 4)
    across = along_x + 4 - 8 * (me // 4)
    local_experts, slot_count, feature_width = inputs_ref.shape
    chips, row_total, width = chips_sum.shape

    def send(source, target, send_sem, recv_sem, device):
        copy = pltpu.make_async_remote_copy(
            src_ref=source,
            dst_ref=target,
            send_sem=send_sem,
            recv_sem=recv_sem,
            device_id=device,
            device_id_type=MESH,
        )
        copy.start()
        return copy

    tok_rows = residual_hbm.shape[0]
    loads = [pltpu.make_async_copy(residual_hbm, blocks.at[me], load_sem.at[0])]
    for index, (hbm, vmem) in enumerate(((gate_hbm, gate_w), (up_hbm, up_w), (down_hbm, down_w))):
        loads.append(pltpu.make_async_copy(hbm, vmem, load_sem.at[index + 1]))
    for copy in loads:
        copy.start()
    load_weight = pltpu.make_async_copy(weight_hbm, weight, load_sem.at[4])
    load_weight.start()

    barrier = pltpu.get_barrier_semaphore()
    peers = [(group, device) for device in (partner, along_x, along_y, across)]
    peers += [((group + d) % groups, me) for d in range(1, groups)]
    for device in peers:
        pl.semaphore_signal(barrier, inc=1, device_id=device, device_id_type=MESH)
    pl.semaphore_wait(barrier, len(peers))

    half, quarter, groups_half = tok_rows // 2, tok_rows // 4, groups // 2
    corner = (me, along_x, along_y, across)

    def block_send_to(index, origin, start, size, device):
        part = blocks.at[origin, pl.ds(start, size)]
        return send(part, part, block_send.at[index], block_recv.at[index], (group, device))

    def row_send_to(index, origin, start, size, device):
        part = rows.at[origin, pl.ds(start, size)]
        return send(part, part, row_send.at[index], row_recv.at[index], (group, device))

    def block_partner(role):
        return block_send_to(8 + role, corner[role], 0, tok_rows, partner)

    def row_partner(role):
        return row_send_to(6 + role, corner[role], 0, groups, partner)

    loads[0].wait()
    block_x0 = block_send_to(0, me, 0, half, along_x)
    block_y0 = block_send_to(1, me, half, half, along_y)
    block_own = block_partner(0)

    for copy in loads[1:]:
        copy.wait()
    contract = (((1,), (1,)), ((), ()))
    for expert in range(local_experts):
        gate_part = lax.dot_general(
            inputs_ref[expert], gate_w[expert], contract, preferred_element_type=jnp.float32
        )
        up_part = lax.dot_general(
            inputs_ref[expert], up_w[expert], contract, preferred_element_type=jnp.float32
        )
        hidden = (gate_part / (1.0 + jnp.exp(-gate_part)) * up_part).astype(jnp.bfloat16)
        lines = pl.ds(expert * slot_count, slot_count)
        for place in range(2 * chips):
            value = jnp.dot(
                hidden,
                down_w[expert, :, place * width : (place + 1) * width],
                preferred_element_type=jnp.float32,
            )
            partial[place, lines, :] = (value * gates_ref[expert]).astype(jnp.bfloat16)

    first = send(
        partial.at[pl.ds((1 - core) * chips, chips)],
        half_in,
        first_send,
        first_recv,
        (group, partner),
    )
    first.wait_recv()
    for chip in range(chips):
        chips_sum[chip] = (
            partial[core * chips + chip].astype(jnp.float32) + half_in[chip].astype(jnp.float32)
        ).astype(jnp.bfloat16)
    reduces = [
        send(
            chips_sum.at[device // 2],
            chips_in.at[index],
            reduce_send.at[index],
            reduce_recv.at[index],
            (group, device),
        )
        for index, device in enumerate((across, along_x, along_y))
    ]
    block_x1 = block_send_to(2, me, half, quarter, along_x)
    block_y1 = block_send_to(3, me, 0, quarter, along_y)
    for copy in reduces:
        copy.wait_recv()
    total = chips_sum[me // 2].astype(jnp.float32)
    for index in range(3):
        total = total + chips_in[index].astype(jnp.float32)
    total = total.astype(jnp.bfloat16)
    for place in range(groups):
        outgoing[place] = jnp.dot(
            table_ref[place], total, preferred_element_type=jnp.float32
        ).astype(jnp.bfloat16)
    exchanges = [
        send(
            outgoing.at[(group + d) % groups],
            rows.at[me, group],
            group_send.at[d - 1],
            group_recv.at[d - 1],
            ((group + d) % groups, me),
        )
        for d in range(1, groups)
    ]
    rows[me, group] = outgoing[group]
    for copy in exchanges:
        copy.wait_recv()
    rest = groups - groups_half
    row_x0 = row_send_to(0, me, 0, groups_half, along_x)
    row_y0 = row_send_to(1, me, groups_half, rest, along_y)
    row_x1 = row_send_to(2, me, groups_half, rest, along_x)
    row_y1 = row_send_to(3, me, 0, groups_half, along_y)
    row_own = row_partner(0)
    row_x0.wait_recv()
    row_ox = row_send_to(4, along_x, 0, groups_half, along_y)
    row_y0.wait_recv()
    row_oy = row_send_to(5, along_y, groups_half, rest, along_x)
    block_x2 = block_send_to(4, me, half + quarter, quarter, along_x)
    block_y2 = block_send_to(5, me, quarter, quarter, along_y)
    block_x0.wait_recv()
    block_ox = block_send_to(6, along_x, 0, half, along_y)
    block_y0.wait_recv()
    block_oy = block_send_to(7, along_y, half, half, along_x)
    row_x1.wait_recv()
    row_px = row_partner(1)
    row_y1.wait_recv()
    row_py = row_partner(2)
    row_ox.wait_recv()
    row_oy.wait_recv()
    row_pd = row_partner(3)
    block_own.wait_recv()
    for copy in (row_own, row_px, row_py, row_pd):
        copy.wait_recv()
    load_weight.wait()

    pair = 2 * tok_rows
    slot_total = slots_ref.shape[1]
    tile = 512
    col_tiles = weight.shape[1] // tile
    stores = []

    def finish_pair(step, chip):
        tokens = lax.broadcasted_iota(jnp.int32, (pair, slot_total), 0) + chip * pair
        placement = jnp.where(slots_ref[...] == tokens, 1.0, 0.0).astype(jnp.bfloat16)

        def place(index, squares):
            cols = pl.ds(pl.multiple_of(index * width, width), width)
            source = (index % chips) * 2 + index // chips
            values = rows[source].reshape(slot_total, width)
            block = blocks[pl.ds(2 * chip, 2), :, cols].reshape(pair, width)
            combined = block.astype(jnp.float32) + jnp.dot(
                placement, values, preferred_element_type=jnp.float32
            )
            combined_ref[:, cols] = combined
            for part in range(0, width, 128):
                piece = combined[:, part : part + 128]
                squares = squares + piece * piece
            return squares

        squares = lax.fori_loop(0, 2 * chips, place, jnp.zeros((pair, 128), jnp.float32), unroll=2)
        scale = lax.rsqrt(jnp.sum(squares, axis=1, keepdims=True) / feature_width + 1e-06)

        def norm(index, carry):
            cols = pl.ds(pl.multiple_of(index * width, width), width)
            normed_ref[:, cols] = (combined_ref[:, cols] * scale * gain_ref[:, cols]).astype(
                jnp.bfloat16
            )
            return carry

        lax.fori_loop(0, 2 * chips, norm, 0, unroll=2)
        if step == 0:
            begin = pl.multiple_of(core * tok_rows, tok_rows)
            stream_ref[...] = combined_ref[pl.ds(begin, tok_rows), :].astype(jnp.bfloat16)

        def project(index, carry):
            cols = pl.ds(pl.multiple_of(index * tile, tile), tile)
            staged[step, :, cols] = jnp.dot(
                normed_ref[...], weight[:, cols], preferred_element_type=jnp.float32
            ).astype(jnp.bfloat16)
            return carry

        lax.fori_loop(0, col_tiles, project, 0)
        begin = pl.multiple_of(chip * pair, pair)
        store = pltpu.make_async_copy(
            staged.at[step], projected_hbm.at[pl.ds(begin, pair)], store_sem.at[step]
        )
        store.start()
        stores.append(store)

    finish_pair(0, me // 2)
    block_x1.wait_recv()
    block_x2.wait_recv()
    block_px = block_partner(1)
    block_y1.wait_recv()
    block_y2.wait_recv()
    block_py = block_partner(2)
    block_px.wait_recv()
    finish_pair(1, along_x // 2)
    block_ox.wait_recv()
    block_oy.wait_recv()
    block_pd = block_partner(3)
    block_py.wait_recv()
    finish_pair(2, along_y // 2)
    block_pd.wait_recv()
    finish_pair(3, across // 2)

    sent = [block_own, block_px, block_py, block_pd, row_own, row_px, row_py, row_pd]
    sent += reduces + exchanges + [first, block_x0, block_x1, block_x2]
    sent += [block_y0, block_y1, block_y2, block_ox, block_oy]
    sent += [row_x0, row_x1, row_y0, row_y1, row_ox, row_oy]
    for copy in sent:
        copy.wait_send()
    for store in stores:
        store.wait()


def communicate(
    groups, members, table, inputs, gates, w_gate, w_up, w_down, residual, slots, gain, w_qkv
):
    local_experts, slot_count, feature_width = inputs.shape
    tok_rows = residual.shape[0]
    row_total = local_experts * slot_count
    width = feature_width // members
    chips = members // 2
    keep = table.shape[1]
    bf16 = jnp.bfloat16
    anywhere = pl.BlockSpec(memory_space=pl.ANY)
    vmem = pl.BlockSpec(memory_space=pltpu.VMEM)
    dma = pltpu.SemaphoreType.DMA
    gate_t, up_t = jnp.swapaxes(w_gate, 1, 2), jnp.swapaxes(w_up, 1, 2)
    return pl.pallas_call(
        functools.partial(comm_kernel, groups),
        in_specs=[vmem] * 3 + [anywhere] * 4 + [vmem, vmem, anywhere],
        out_specs=[vmem, anywhere],
        out_shape=[
            jax.ShapeDtypeStruct((tok_rows, feature_width), bf16),
            jax.ShapeDtypeStruct((members * tok_rows, w_qkv.shape[1]), bf16),
        ],
        scratch_shapes=[
            pltpu.VMEM(gate_t.shape, bf16),
            pltpu.VMEM(up_t.shape, bf16),
            pltpu.VMEM(w_down.shape, bf16),
            pltpu.VMEM(w_qkv.shape, bf16),
            pltpu.VMEM((members, tok_rows, feature_width), bf16),
            pltpu.VMEM((members, groups, keep, width), bf16),
            pltpu.VMEM((2 * tok_rows, feature_width), jnp.float32),
            pltpu.VMEM((2 * tok_rows, feature_width), bf16),
            pltpu.VMEM((chips, 2 * tok_rows, w_qkv.shape[1]), bf16),
            pltpu.VMEM((members, row_total, width), bf16),
            pltpu.VMEM((chips, row_total, width), bf16),
            pltpu.VMEM((chips, row_total, width), bf16),
            pltpu.VMEM((chips - 1, row_total, width), bf16),
            pltpu.VMEM((groups, keep, width), bf16),
            dma((5,)),
            dma,
            dma,
            dma((3,)),
            dma((3,)),
            dma((groups - 1,)),
            dma((groups - 1,)),
            dma((12,)),
            dma((12,)),
            dma((10,)),
            dma((10,)),
            dma((chips,)),
        ],
        compiler_params=pltpu.CompilerParams(
            collective_id=0, has_side_effects=True, vmem_limit_bytes=60 * 1024 * 1024
        ),
    )(inputs, gates[:, :, None], table, gate_t, up_t, w_down, residual, slots, gain, w_qkv)


def plain_rows(
    expert_inputs, gates, w_gate, w_up, w_down, send_table, expert_count, tensor_count
):
    local_experts, slot_count, feature_width = expert_inputs.shape
    gate_part = jnp.einsum(
        "ecd,edf->ecf", expert_inputs, w_gate, preferred_element_type=jnp.float32
    )
    up_part = jnp.einsum("ecd,edf->ecf", expert_inputs, w_up, preferred_element_type=jnp.float32)
    hidden = (jax.nn.silu(gate_part) * up_part).astype(jnp.bfloat16)
    partial_value = (
        jnp.einsum("ecf,efd->ecd", hidden, w_down, preferred_element_type=jnp.float32)
        * gates[:, :, None]
    ).astype(jnp.bfloat16)
    row_total = local_experts * slot_count
    arrived = lax.all_to_all(
        partial_value.reshape(row_total, feature_width),
        "tensor",
        split_axis=1,
        concat_axis=0,
        tiled=True,
    ).reshape(tensor_count, local_experts, slot_count, -1)
    summed = jnp.sum(arrived.astype(jnp.float32), axis=0).astype(jnp.bfloat16)

    outgoing = jnp.einsum("zlkmj,mjf->zlkf", send_table, summed)
    incoming = lax.all_to_all(
        outgoing.reshape(expert_count, -1, outgoing.shape[-1]),
        "expert",
        split_axis=0,
        concat_axis=0,
        tiled=True,
    )
    incoming = incoming.reshape(-1, outgoing.shape[-1])
    return lax.all_gather(incoming, "tensor", axis=0, tiled=False)


def per_device(
    expert_inputs, gates, chosen_tokens, w_gate, w_up, w_down, residual, norm_gain, w_qkv
):
    expert_count = lax.axis_size("expert")
    tensor_count = lax.axis_size("tensor")
    my_group = lax.axis_index("expert")
    local_experts, slot_count, feature_width = expert_inputs.shape
    tok_rows = residual.shape[0]
    group_rows = tok_rows * tensor_count
    keep = min(slot_count, MOST * tensor_count)

    dest = chosen_tokens // group_rows
    earlier = jnp.arange(slot_count)[None, :] < jnp.arange(slot_count)[:, None]
    rank = jnp.sum(
        ((dest[:, :, None] == dest[:, None, :]) & earlier[None]).astype(jnp.int32), axis=2
    )
    kept = jnp.arange(keep, dtype=jnp.int32)
    mine = jnp.where(dest == my_group, rank, -1)
    token_at = jnp.sum(
        jnp.where(
            mine[:, None, :] == kept[None, :, None],
            (chosen_tokens % group_rows)[:, None, :] + 1,
            0,
        ),
        axis=2,
    ).reshape(1, -1) - 1

    local_dest = lax.dynamic_slice_in_dim(dest, my_group * local_experts, local_experts, 0)
    local_rank = lax.dynamic_slice_in_dim(rank, my_group * local_experts, local_experts, 0)
    send_table = (
        (local_dest[None, :, None, :] == jnp.arange(expert_count)[:, None, None, None])
        & (local_rank[None, :, None, :] == kept[None, None, :, None])
    ).astype(jnp.bfloat16)
    same = jnp.eye(local_experts, dtype=jnp.bfloat16)
    send_table = send_table[:, :, :, None, :] * same[None, :, None, :, None]
    if tensor_count == 8:
        return communicate(
            expert_count,
            tensor_count,
            send_table.reshape(expert_count, local_experts * keep, -1),
            expert_inputs,
            gates,
            w_gate,
            w_up,
            w_down,
            residual,
            token_at,
            norm_gain[None, :],
            w_qkv,
        )
    residual_all = lax.all_gather(residual, "tensor", axis=0, tiled=True)
    rows = plain_rows(
        expert_inputs, gates, w_gate, w_up, w_down, send_table, expert_count, tensor_count
    )
    order = tuple(range(tensor_count))
    return finish(
        lax.axis_index("tensor").reshape(1),
        token_at,
        residual_all,
        rows,
        order,
        norm_gain[None, :],
        w_qkv,
        tok_rows,
    )


def solution(mesh):
    return jax.shard_map(
        per_device,
        mesh=mesh,
        in_specs=(
            P("expert", None, None),
            P("expert", None),
            P(),
            P("expert", None, "tensor"),
            P("expert", None, "tensor"),
            P("expert", "tensor", None),
            P(("expert", "tensor"), None),
            P(),
            P(None, "tensor"),
        ),
        out_specs=(P(("expert", "tensor"), None), P("expert", "tensor")),
        check_vma=False,
    )
```
